32 devices in a mesh: samp: 4 (over x, core), snp: 8 (over z, y).
Axes of the slice: x: 2, y: 2, z: 4, core: 2. Of those that a mesh axis runs over, the one named last changes fastest.
Arguments:
- genotypes: float32 [4096, 8192], P('samp', 'snp'), may hold values from -1 to 2, as said below
Outputs:
- band_r: float32 [8192, 4096], P('snp', 'samp')
The draws below stay inside these ranges and needn't reach their ends.
Inputs may be any that keep to these rules, and one draw needn't show every extreme that they name: `genotypes`: -1 marks a missing dosage; every other value lies between 0 and 2. Every eighth sample (samples 0, 8, 16, ...) has no missing dosage, and over those samples each SNP's dosages run through 0, 1, 2 cyclically from a SNP's own starting value.
All inputs are finite; a program needn't handle non-finite values.
Results may differ from the reference program's by a relative error of at most 0.006.
Values may be sent and summed in bfloat16 or wider, within the bound.
A program may use at most 64 MiB of HBM per device.

```python
import jax
import jax.numpy as jnp
from jax import lax

TILE = 512
BAND = 4096
NSAMP = 4096
NSNP = 8192


def draw_genotypes(key, part):
    window = 32
    key_bits = jax.random.fold_in(key, 11)
    key_offset = jax.random.fold_in(key, 12)
    key_cycle = jax.random.fold_in(key, 13)
    key_missing = jax.random.fold_in(key, 14)
    key_jitter = jax.random.fold_in(key, 15)
    bits = jax.random.randint(key_bits, (NSAMP, NSNP + window), 0, 2, dtype=jnp.int32)
    running = jnp.cumsum(bits, axis=1)
    window_sum = running[:, window:] - running[:, :-window]
    offset = jax.random.randint(key_offset, (NSNP,), -4, 5, dtype=jnp.int32)
    sample_row = jnp.arange(NSAMP, dtype=jnp.int32)
    drift = 6 * sample_row // NSAMP
    level = (window_sum + offset[None, :] + drift[:, None]).astype(jnp.float32)
    jitter = jax.random.uniform(key_jitter, (NSAMP, NSNP), jnp.float32, 0.0, 1.0)
    temper = 2.0
    dosage = 2.0 * jax.nn.sigmoid((level + jitter - 19.0) / temper)
    cycle_start = jax.random.randint(key_cycle, (NSNP,), 0, 3, dtype=jnp.int32)
    anchor = (sample_row % 8 == 0)[:, None]
    cycled = ((sample_row[:, None] // 8 + cycle_start[None, :]) % 3).astype(jnp.float32)
    dosage = jnp.where(anchor, cycled, dosage)
    percent = 3 + 9 * sample_row // NSAMP
    missing_roll = jax.random.randint(key_missing, (NSAMP, NSNP), 0, 100, dtype=jnp.int32)
    missing = (missing_roll < percent[:, None]) & jnp.logical_not(anchor)
    return jnp.where(missing, -1.0, dosage).astype(jnp.float32)


def setup_inputs(seed: int = 0) -> dict:
    splits = jax.random.split(jax.random.key(seed), 2)
    genotypes = draw_genotypes(jax.random.fold_in(splits[1], 71), 0)
    return dict(genotypes=genotypes)


EPS = 1e-05

def reference(genotypes):
    present = (genotypes >= 0).astype(jnp.float32)
    dosage = genotypes.astype(jnp.float32) * present
    counted = lax.optimization_barrier(jnp.sum(present, axis=0))
    summed = lax.optimization_barrier(jnp.sum(dosage, axis=0))
    squared = lax.optimization_barrier(jnp.sum(dosage * dosage, axis=0))
    average = summed / counted
    spread = squared / counted - average * average
    scaled = (present * (dosage - average) * lax.rsqrt(spread + EPS)).astype(jnp.bfloat16)
    col_norms = counted * spread / (spread + EPS)
    total_snps = genotypes.shape[1]
    padded = jnp.concatenate([scaled, jnp.zeros((scaled.shape[0], BAND), scaled.dtype)], axis=1)
    padded_norms = jnp.concatenate([col_norms, jnp.ones((BAND,), jnp.float32)])

    def band_tile(tile_pos):
        start = (tile_pos * TILE).astype(jnp.int32)
        row_block = lax.dynamic_slice_in_dim(scaled, start, TILE, 1)
        col_block = lax.dynamic_slice_in_dim(padded, start, BAND, 1)
        products = lax.dot_general(row_block, col_block, (((0,), (0,)), ((), ())), preferred_element_type=jnp.float32)
        row_norm = lax.dynamic_slice_in_dim(col_norms, start, TILE, 0)
        col_norm = lax.dynamic_slice_in_dim(padded_norms, start, BAND, 0)
        return products / jnp.sqrt(row_norm[:, None] * col_norm[None, :])
    tiles = lax.map(band_tile, jnp.arange(total_snps // TILE, dtype=jnp.int32))
    return tiles.reshape(total_snps, BAND)
```

```python
import jax
import jax.numpy as jnp
from jax import lax
from jax.sharding import PartitionSpec as P

TILE = 512
BAND = 4096
EPS = 1e-05


def exchanged(x, axis, mask):
    count = lax.axis_size(axis)
    return lax.ppermute(x, axis, [(i, i ^ mask) for i in range(count)])


def product(rows, cols):
    return lax.dot_general(
        rows, cols, (((0,), (0,)), ((), ())), preferred_element_type=jnp.float32
    )


def on_device(genotypes):
    present = (genotypes >= 0).astype(jnp.float32)
    dosage = genotypes * present
    stats = jnp.stack(
        [jnp.sum(present, axis=0), jnp.sum(dosage, axis=0), jnp.sum(dosage * dosage, axis=0)]
    )
    stats = stats + exchanged(stats, "samp", 1)
    stats = stats + exchanged(stats, "samp", 2)
    counted, summed, squared = stats[0], stats[1], stats[2]
    average = summed / counted
    spread = squared / counted - average * average
    col_norms = counted * spread / (spread + EPS)
    factor = lax.rsqrt(spread + EPS) * lax.rsqrt(col_norms)
    scaled = (present * (dosage - average) * factor).astype(jnp.bfloat16)

    half = genotypes.shape[1] // 2
    assert half == TILE and BAND == 8 * half
    count = lax.axis_size("snp")
    assert count % 2 == 0 and lax.axis_size("samp") == 4
    odd_down = [(i, i - 1) for i in range(1, count, 2)]
    even_up = [(i, i + 1) for i in range(0, count, 2)]
    two_down = [(i, i - 2) for i in range(2, count)]
    odd_two_down = [(i, i - 2) for i in range(3, count, 2)]
    odd = lax.axis_index("snp") % 2 == 1

    own0, own1 = scaled[:, :half], scaled[:, half:]
    z0 = lax.ppermute(own0, "snp", two_down)
    a0 = lax.ppermute(own0, "snp", odd_down)
    z1 = lax.ppermute(own1, "snp", two_down)
    a1 = lax.ppermute(own1, "snp", odd_down)
    y0 = lax.ppermute(z0, "snp", even_up + odd_down)
    y1 = lax.ppermute(z1, "snp", even_up + odd_down)
    d0 = lax.ppermute(z0, "snp", two_down)
    e0 = lax.ppermute(d0, "snp", even_up)
    e1 = lax.ppermute(y1, "snp", odd_two_down)

    samp = lax.axis_index("samp")
    core = samp % 2
    keep_rows = lax.dynamic_slice_in_dim(scaled, core * half, half, 1)
    send_rows = lax.dynamic_slice_in_dim(scaled, (1 - core) * half, half, 1)

    def chip_sum(cols, pairs):
        given = product(send_rows, cols).astype(jnp.bfloat16)
        got = lax.ppermute(given, "samp", pairs)
        return (product(keep_rows, cols) + got.astype(jnp.float32)).astype(jnp.bfloat16)

    def whole_sum(part, pairs):
        return part + lax.ppermute(part, "samp", pairs)

    swap = [(0, 1), (1, 0), (2, 3), (3, 2)]
    to_low = [(2, 0), (3, 1)]
    to_high = [(0, 2), (1, 3)]
    cat = lambda *xs: jnp.concatenate(xs, axis=1)
    s = [None] * 9
    r01 = chip_sum(scaled, swap)
    w01 = whole_sum(r01, to_low)
    s[0], s[1] = w01[:, :half], w01[:, half:]
    r4 = chip_sum(z0, swap)
    r5 = chip_sum(z1, swap)
    s[4] = whole_sum(r4, [(0, 2), (3, 1)])
    s[5] = whole_sum(r5, to_high)
    s[2] = whole_sum(chip_sum(jnp.where(odd, y0, a0), swap), to_low)
    s[3] = whole_sum(chip_sum(jnp.where(odd, y1, a1), swap), to_low)
    s[8] = whole_sum(chip_sum(d0, [(0, 1), (2, 3)]), [(1, 3)])
    s[6] = whole_sum(chip_sum(jnp.where(odd, e0, y0), swap), to_high)
    s[7] = whole_sum(chip_sum(jnp.where(odd, e1, y1), swap), to_high)

    def chosen(options):
        parts = [cat(s[i], s[j]) for i, j in options]
        return jnp.where(
            samp < 2,
            jnp.where(samp == 0, parts[0], parts[1]),
            jnp.where(samp == 2, parts[2], parts[3]),
        )

    sent = chosen([(2, 3), (1, 2), (6, 7), (5, 6)])
    kept = chosen([(0, 1), (3, 4), (4, 5), (7, 8)])
    got = exchanged(sent, "samp", 1)
    first = jnp.where(core == 0, kept, got)
    second = jnp.where(core == 0, got, kept)
    return jnp.concatenate([first, second], axis=0).astype(jnp.float32)


def solution(mesh):
    return jax.shard_map(
        on_device, mesh=mesh, in_specs=(P("samp", "snp"),), out_specs=P("snp", "samp"),
        check_vma=False,
    )
```

```python
import jax
import jax.numpy as jnp
from jax import lax
from jax.experimental import pallas as pl
from jax.experimental.pallas import tpu as pltpu
from jax.sharding import PartitionSpec as P

TILE = 512
BAND = 4096
EPS = 1e-05
MESH = pl.DeviceIdType.MESH


def exchanged(x, axis, mask):
    count = lax.axis_size(axis)
    return lax.ppermute(x, axis, [(i, i ^ mask) for i in range(count)])


def band_kernel(
    count, own, keep_rows, send_rows, out,
    panels, given, got, part, far, passed,
    panel_send, panel_recv, given_send, got_recv, part_send, far_recv, final_send, final_recv,
):
    p, samp = lax.axis_index("snp"), lax.axis_index("samp")
    core, x = samp % 2, samp // 2
    core_peer = samp + 1 - 2 * core
    x_peer = samp + 2 - 4 * x
    odd = p % 2 == 1
    even = p % 2 == 0
    mate = p + 1 - 2 * (p % 2)
    has_down = p >= 2
    has_up = p + 2 < count

    barrier = pltpu.get_barrier_semaphore()

    def greet(where):
        pl.semaphore_signal(barrier, inc=1, device_id=where, device_id_type=MESH)

    greet({"samp": core_peer})
    greet({"samp": x_peer})
    greet({"snp": mate})

    @pl.when(has_down)
    def _():
        greet({"snp": p - 2})

    @pl.when(has_up)
    def _():
        greet({"snp": p + 2})

    peers = 3 + has_down.astype(jnp.int32) + has_up.astype(jnp.int32)
    pl.semaphore_wait(barrier, peers)

    def block(h):
        return own.at[h] if h < 2 else panels.at[h - 2]

    def valid(h):
        return p + h // 2 < count

    def panel_copy(n, source, target, where):
        return pltpu.make_async_remote_copy(
            src_ref=block(source), dst_ref=panels.at[target - 2],
            send_sem=panel_send.at[n], recv_sem=panel_recv.at[target - 2],
            device_id={"snp": where}, device_id_type=MESH,
        )

    sends = {
        "z0": (0, has_down, 0, 4, p - 2),
        "z1": (1, has_down, 1, 5, p - 2),
        "a0": (2, odd, 0, 2, mate),
        "a1": (3, odd, 1, 3, mate),
        "y0e": (4, even & has_up, 4, 2, mate),
        "y0o": (4, odd & has_up, 4, 6, mate),
        "y1e": (5, even & has_up, 5, 3, mate),
        "y1o": (5, odd & has_up, 5, 7, mate),
        "d0": (6, has_down & has_up, 4, 8, p - 2),
        "e0": (7, even & (p + 4 < count), 8, 6, mate),
        "e1": (8, odd & has_down & (p + 1 < count), 3, 7, p - 2),
    }

    def send(name):
        n, cond, source, target, where = sends[name]

        @pl.when(cond)
        def _():
            panel_copy(n, source, target, where).start()

    def arrived(h):
        @pl.when(valid(h))
        def _():
            panel_copy(0, 0, h, mate).wait_recv()

    def keeps(h):
        return valid(h) & {0: core == 0, 8: core == 1}.get(h, core >= 0)

    def gives(h):
        return valid(h) & {0: core == 1, 8: core == 0}.get(h, core >= 0)

    def given_copy(h):
        return pltpu.make_async_remote_copy(
            src_ref=given.at[h], dst_ref=got.at[h],
            send_sem=given_send.at[h], recv_sem=got_recv.at[h],
            device_id={"samp": core_peer}, device_id_type=MESH,
        )

    def part_copy(h):
        return pltpu.make_async_remote_copy(
            src_ref=part.at[h], dst_ref=far.at[h],
            send_sem=part_send.at[h], recv_sem=far_recv.at[h],
            device_id={"samp": x_peer}, device_id_type=MESH,
        )

    step = 256
    steps = keep_rows.shape[0] // step

    def first(h):
        @pl.when(gives(h))
        def _():
            @pl.loop(0, steps)
            def _(r):
                rows = pl.ds(pl.multiple_of(r * step, step), step)
                given[h, rows, :] = jnp.dot(
                    send_rows[rows, :], block(h)[...], preferred_element_type=jnp.float32
                ).astype(given.dtype)

            given_copy(h).start()

    def owner(h):
        return (h - core) // 4

    def second(h):
        @pl.when(keeps(h))
        def _():
            given_copy(h).wait_recv()

            @pl.loop(0, steps)
            def _(r):
                rows = pl.ds(pl.multiple_of(r * step, step), step)
                value = jnp.dot(
                    keep_rows[rows, :], block(h)[...], preferred_element_type=jnp.float32
                )
                part[h, rows, :] = (value + got[h, rows, :].astype(jnp.float32)).astype(part.dtype)

            @pl.when(owner(h) != x)
            def _():
                part_copy(h).start()

    def final_copy(j):
        return pltpu.make_async_remote_copy(
            src_ref=passed.at[j], dst_ref=out.at[core, j],
            send_sem=final_send.at[j], recv_sem=final_recv.at[j],
            device_id={"samp": core_peer}, device_id_type=MESH,
        )

    def third(h):
        for c in (0, 1):
            i = (h - c) % 4
            j = i % 2
            stays = (i < 2) == (c == 0)
            if not 0 <= h - c < 8:
                continue
            mine = (core == c) & (owner(h) == x)

            def total(target, at, i=i):
                @pl.when(mine & valid(h))
                def _():
                    part_copy(h).wait_recv()
                    target[at] = (
                        part[h].astype(jnp.float32) + far[h].astype(jnp.float32)
                    ).astype(target.dtype)

                @pl.when(mine & jnp.logical_not(valid(h)))
                def _():
                    target[at] = jnp.zeros(target.shape[-2:], target.dtype)

            if stays:
                total(out, (c, j))
            else:
                total(passed, (j,))

                @pl.when(mine)
                def _(j=j):
                    final_copy(j).start()

    for name in ("z0", "a0", "z1", "a1"):
        send(name)
    first(0)
    first(1)
    second(0)
    second(1)
    arrived(4)
    for name in ("y0e", "y0o", "d0"):
        send(name)
    first(4)
    second(4)
    arrived(5)
    for name in ("y1e", "y1o"):
        send(name)
    first(5)
    second(5)
    arrived(2)
    first(2)
    second(2)
    arrived(3)
    send("e1")
    first(3)
    arrived(8)
    send("e0")
    first(8)
    second(3)
    second(8)
    for h in (0, 1, 2):
        third(h)
    arrived(6)
    first(6)
    second(6)
    arrived(7)
    first(7)
    second(7)
    for h in (3, 4, 5, 8, 6, 7):
        third(h)

    for j in (0, 1):
        final_copy(j).wait_recv()
        final_copy(j).wait_send()
    for n, cond, source, target, where in sends.values():
        @pl.when(cond)
        def _(n=n, source=source, target=target, where=where):
            panel_copy(n, source, target, where).wait_send()
    for h in range(9):
        @pl.when(gives(h))
        def _(h=h):
            given_copy(h).wait_send()

        @pl.when(keeps(h) & (owner(h) != x))
        def _(h=h):
            part_copy(h).wait_send()


def on_device(genotypes):
    present = (genotypes >= 0).astype(jnp.float32)
    dosage = genotypes * present
    stats = jnp.stack(
        [jnp.sum(present, axis=0), jnp.sum(dosage, axis=0), jnp.sum(dosage * dosage, axis=0)]
    )
    stats = stats + exchanged(stats, "samp", 1)
    stats = stats + exchanged(stats, "samp", 2)
    counted, summed, squared = stats[0], stats[1], stats[2]
    average = summed / counted
    spread = squared / counted - average * average
    col_norms = counted * spread / (spread + EPS)
    factor = lax.rsqrt(spread + EPS) * lax.rsqrt(col_norms)
    scaled = (present * (dosage - average) * factor).astype(jnp.bfloat16)

    samples, snps = genotypes.shape
    half = snps // 2
    count = lax.axis_size("snp")
    assert half == TILE and BAND == 8 * half
    assert count % 2 == 0 and lax.axis_size("samp") == 4
    core = lax.axis_index("samp") % 2
    own = jnp.stack([scaled[:, :half], scaled[:, half:]])
    flipped = scaled.T
    keep_rows = lax.dynamic_slice_in_dim(flipped, core * half, half, 0)
    send_rows = lax.dynamic_slice_in_dim(flipped, (1 - core) * half, half, 0)

    piece = lambda n: pltpu.VMEM((n, half, half), jnp.bfloat16)
    sems = lambda n: pltpu.SemaphoreType.DMA((n,))
    vmem = pl.BlockSpec(memory_space=pltpu.VMEM)
    out = pl.pallas_call(
        lambda *refs: band_kernel(count, *refs),
        out_shape=jax.ShapeDtypeStruct((2, 2, half, half), jnp.bfloat16),
        in_specs=[vmem] * 3,
        out_specs=vmem,
        scratch_shapes=[
            pltpu.VMEM((7, samples, half), jnp.bfloat16),
            piece(9), piece(9), piece(9), piece(9), piece(2),
            sems(9), sems(7), sems(9), sems(9), sems(9), sems(9), sems(2), sems(2),
        ],
        compiler_params=pltpu.CompilerParams(
            collective_id=0, has_side_effects=True, vmem_limit_bytes=60 * 1024 * 1024
        ),
    )(own, keep_rows, send_rows)
    return out.transpose(0, 2, 1, 3).reshape(snps, snps).astype(jnp.float32)


def solution(mesh):
    return jax.shard_map(
        on_device, mesh=mesh, in_specs=(P("samp", "snp"),), out_specs=P("snp", "samp"),
        check_vma=False,
    )
```

```python
import jax
import jax.numpy as jnp
from jax import lax
from jax.experimental import pallas as pl
from jax.experimental.pallas import tpu as pltpu
from jax.sharding import PartitionSpec as P

TILE = 512
BAND = 4096
EPS = 1e-05
MESH = pl.DeviceIdType.MESH


def exchanged(x, axis, mask):
    count = lax.axis_size(axis)
    return lax.ppermute(x, axis, [(i, i ^ mask) for i in range(count)])


def band_kernel(
    count, own, keep_rows, send_rows, out,
    panels, given, got, part, far, passed,
    panel_send, panel_recv, given_send, got_recv, part_send, far_recv, final_send, final_recv,
):
    p, samp = lax.axis_index("snp"), lax.axis_index("samp")
    core, x = samp % 2, samp // 2
    core_peer = samp + 1 - 2 * core
    x_peer = samp + 2 - 4 * x
    odd = p % 2 == 1
    even = p % 2 == 0
    mate = p + 1 - 2 * (p % 2)
    has_down = p >= 2
    has_up = p + 2 < count

    barrier = pltpu.get_barrier_semaphore()

    def greet(where):
        pl.semaphore_signal(barrier, inc=1, device_id=where, device_id_type=MESH)

    greet({"samp": core_peer})
    greet({"samp": x_peer})
    greet({"snp": mate})

    @pl.when(has_down)
    def _():
        greet({"snp": p - 2})

    @pl.when(has_up)
    def _():
        greet({"snp": p + 2})

    peers = 3 + has_down.astype(jnp.int32) + has_up.astype(jnp.int32)
    pl.semaphore_wait(barrier, peers)

    def block(h):
        return own.at[h] if h < 2 else panels.at[h - 2]

    def valid(h):
        return p + h // 2 < count

    def panel_copy(n, source, target, where):
        return pltpu.make_async_remote_copy(
            src_ref=block(source), dst_ref=panels.at[target - 2],
            send_sem=panel_send.at[n], recv_sem=panel_recv.at[target - 2],
            device_id={"snp": where}, device_id_type=MESH,
        )

    sends = {
        "z0": (0, has_down, 0, 4, p - 2),
        "z1": (1, has_down, 1, 5, p - 2),
        "a0": (2, odd, 0, 2, mate),
        "a1": (3, odd, 1, 3, mate),
        "y0e": (4, even & has_up, 4, 2, mate),
        "y0o": (4, odd & has_up, 4, 6, mate),
        "y1e": (5, even & has_up, 5, 3, mate),
        "y1o": (5, odd & has_up, 5, 7, mate),
        "d0": (6, has_down & has_up, 4, 8, p - 2),
        "e0": (7, even & (p + 4 < count), 8, 6, mate),
        "e1": (8, odd & has_down & (p + 1 < count), 3, 7, p - 2),
    }

    def send(name):
        n, cond, source, target, where = sends[name]

        @pl.when(cond)
        def _():
            panel_copy(n, source, target, where).start()

    def arrived(h):
        @pl.when(valid(h))
        def _():
            panel_copy(0, 0, h, mate).wait_recv()

    def keeps(h):
        return valid(h) & {0: core == 0, 8: core == 1}.get(h, core >= 0)

    def gives(h):
        return valid(h) & {0: core == 1, 8: core == 0}.get(h, core >= 0)

    def given_copy(h):
        return pltpu.make_async_remote_copy(
            src_ref=given.at[h], dst_ref=got.at[h],
            send_sem=given_send.at[h], recv_sem=got_recv.at[h],
            device_id={"samp": core_peer}, device_id_type=MESH,
        )

    def part_copy(h):
        return pltpu.make_async_remote_copy(
            src_ref=part.at[h], dst_ref=far.at[h],
            send_sem=part_send.at[h], recv_sem=far_recv.at[h],
            device_id={"samp": x_peer}, device_id_type=MESH,
        )

    half = keep_rows.shape[0]
    step = 256
    steps = half // step

    def first(h):
        @pl.when(gives(h))
        def _():
            @pl.loop(0, steps)
            def _(r):
                rows = pl.ds(pl.multiple_of(r * step, step), step)
                given[h, rows, :] = jnp.dot(
                    send_rows[rows, :], block(h)[...], preferred_element_type=jnp.float32
                ).astype(given.dtype)

            given_copy(h).start()

    def owner(h):
        return (h - core) // 4

    def second(h):
        @pl.when(keeps(h))
        def _():
            given_copy(h).wait_recv()

            @pl.loop(0, steps)
            def _(r):
                rows = pl.ds(pl.multiple_of(r * step, step), step)
                value = jnp.dot(
                    keep_rows[rows, :], block(h)[...], preferred_element_type=jnp.float32
                )
                part[h, rows, :] = (value + got[h, rows, :].astype(jnp.float32)).astype(part.dtype)

            @pl.when(owner(h) != x)
            def _():
                part_copy(h).start()

    def final_copy(j):
        return pltpu.make_async_remote_copy(
            src_ref=passed.at[j], dst_ref=out.at[core, :, pl.ds(j * half, half)],
            send_sem=final_send.at[j], recv_sem=final_recv.at[j],
            device_id={"samp": core_peer}, device_id_type=MESH,
        )

    def third(h):
        for c in (0, 1):
            i = (h - c) % 4
            j = i % 2
            stays = (i < 2) == (c == 0)
            if not 0 <= h - c < 8:
                continue
            mine = (core == c) & (owner(h) == x)

            def total(target, at, i=i):
                @pl.when(mine & valid(h))
                def _():
                    part_copy(h).wait_recv()
                    target[at] = (
                        part[h].astype(jnp.float32) + far[h].astype(jnp.float32)
                    ).astype(target.dtype)

                @pl.when(mine & jnp.logical_not(valid(h)))
                def _():
                    target[at] = jnp.zeros(part.shape[1:], target.dtype)

            if stays:
                total(out, (c, slice(None), pl.ds(j * half, half)))
            else:
                total(passed, (j,))

                @pl.when(mine)
                def _(j=j):
                    final_copy(j).start()

    for name in ("z0", "a0", "z1", "a1"):
        send(name)
    first(0)
    first(1)
    second(0)
    second(1)
    arrived(4)
    for name in ("y0e", "y0o", "d0"):
        send(name)
    first(4)
    second(4)
    arrived(5)
    for name in ("y1e", "y1o"):
        send(name)
    first(5)
    second(5)
    arrived(2)
    first(2)
    second(2)
    arrived(3)
    send("e1")
    first(3)
    arrived(8)
    send("e0")
    first(8)
    second(3)
    second(8)
    for h in (0, 1, 2):
        third(h)
    arrived(6)
    first(6)
    second(6)
    arrived(7)
    first(7)
    second(7)
    for h in (3, 4, 5, 8, 6, 7):
        third(h)

    for j in (0, 1):
        final_copy(j).wait_recv()
        final_copy(j).wait_send()
    for n, cond, source, target, where in sends.values():
        @pl.when(cond)
        def _(n=n, source=source, target=target, where=where):
            panel_copy(n, source, target, where).wait_send()
    for h in range(9):
        @pl.when(gives(h))
        def _(h=h):
            given_copy(h).wait_send()

        @pl.when(keeps(h) & (owner(h) != x))
        def _(h=h):
            part_copy(h).wait_send()


def on_device(genotypes):
    present = (genotypes >= 0).astype(jnp.float32)
    dosage = genotypes * present
    stats = jnp.stack(
        [jnp.sum(present, axis=0), jnp.sum(dosage, axis=0), jnp.sum(dosage * dosage, axis=0)]
    )
    stats = stats + exchanged(stats, "samp", 1)
    stats = stats + exchanged(stats, "samp", 2)
    counted, summed, squared = stats[0], stats[1], stats[2]
    average = summed / counted
    spread = squared / counted - average * average
    col_norms = counted * spread / (spread + EPS)
    factor = lax.rsqrt(spread + EPS) * lax.rsqrt(col_norms)
    scaled = (present * (dosage - average) * factor).astype(jnp.bfloat16)

    samples, snps = genotypes.shape
    half = snps // 2
    count = lax.axis_size("snp")
    assert half == TILE and BAND == 8 * half
    assert count % 2 == 0 and lax.axis_size("samp") == 4
    core = lax.axis_index("samp") % 2
    own = jnp.stack([scaled[:, :half], scaled[:, half:]])
    flipped = scaled.T
    keep_rows = lax.dynamic_slice_in_dim(flipped, core * half, half, 0)
    send_rows = lax.dynamic_slice_in_dim(flipped, (1 - core) * half, half, 0)

    piece = lambda n: pltpu.VMEM((n, half, half), jnp.bfloat16)
    sems = lambda n: pltpu.SemaphoreType.DMA((n,))
    vmem = pl.BlockSpec(memory_space=pltpu.VMEM)
    out = pl.pallas_call(
        lambda *refs: band_kernel(count, *refs),
        out_shape=jax.ShapeDtypeStruct((2, half, snps), jnp.bfloat16),
        in_specs=[vmem] * 3,
        out_specs=vmem,
        scratch_shapes=[
            pltpu.VMEM((7, samples, half), jnp.bfloat16),
            piece(9), piece(9), piece(9), piece(9), piece(2),
            sems(9), sems(7), sems(9), sems(9), sems(9), sems(9), sems(2), sems(2),
        ],
        compiler_params=pltpu.CompilerParams(
            collective_id=0, has_side_effects=True, vmem_limit_bytes=60 * 1024 * 1024
        ),
    )(own, keep_rows, send_rows)
    return out.reshape(snps, snps).astype(jnp.float32)


def solution(mesh):
    return jax.shard_map(
        on_device, mesh=mesh, in_specs=(P("samp", "snp"),), out_specs=P("snp", "samp"),
        check_vma=False,
    )
```
